512 devices in a mesh: ctx: 64 (over y, z_hi, x), tp: 8 (over z_lo, core).
Axes of the slice: x: 4, y: 4, z: 16 (z_hi: 4, z_lo: 4; z = z_hi * 4 + z_lo), core: 2. Of those that a mesh axis runs over, the one named last changes fastest.
Arguments:
- queries: bfloat16 [8192, 4096], P('ctx', 'tp'), may hold values from -220 to 220
- keys: bfloat16 [8192, 1024], P('ctx', 'tp'), may hold values from -6 to 6
- values: bfloat16 [8192, 1024], P('ctx', 'tp'), may hold values from -6 to 6
- out_weight: bfloat16 [4096, 4096], P('tp'), may hold values from -0.09375 to 0.09375
- residual: bfloat16 [8192, 4096], P('ctx', 'tp'), may hold values from -1.5 to 1.5
- norm_gain: bfloat16 [4096], P('tp'), may hold values from 0.5 to 1.5
- span_order: int32 [128], replicated, may hold values from 0 to 127, as said below
Outputs:
- normed: bfloat16 [8192, 4096], P('ctx', 'tp')
The draws below stay inside these ranges and needn't reach their ends.
Inputs may be any that keep to these rules, and one draw needn't show every extreme that they name: `span_order`: every span appears in exactly one slot. The two slots of one index d of ctx (slots 2d and 2d + 1) hold a span p and its mirror, the span at the same place counted from the end of the sequence; which index holds which pair, and the order of the two, are drawn.
All inputs are finite; a program needn't handle non-finite values.
Results may differ from the reference program's by a relative error of at most 0.009.
Values may be sent and summed in bfloat16 or wider, within the bound.
No kernel may reach another device: no remote copies, remote signals or barrier semaphores. Data moves between devices by JAX's collectives and lax.ppermute only.
A program may use at most 64 MiB of HBM per device.

```python
import math
import jax
import jax.numpy as jnp
from jax import lax

D = 4096
QUERY_HEADS = 32
KEY_VALUE_HEADS = 8
HEAD_SIZE = 128
SEQUENCE_LENGTH = 8192
N_CTX = 64


def paired_draw(key):
    base = jax.random.fold_in(key, 4242)
    query_key, random_key_seed = jax.random.split(base)
    query_raw = jnp.clip(jax.random.normal(query_key, (SEQUENCE_LENGTH, QUERY_HEADS, HEAD_SIZE), jnp.float32), -6.0, 6.0)
    key_input_rows = jnp.clip(jax.random.normal(random_key_seed, (SEQUENCE_LENGTH, KEY_VALUE_HEADS, HEAD_SIZE), jnp.float32), -6.0, 6.0)
    key_output_rows = key_input_rows
    query_output_rows = query_raw
    return (query_output_rows.reshape(SEQUENCE_LENGTH, QUERY_HEADS * HEAD_SIZE), key_output_rows.reshape(SEQUENCE_LENGTH, KEY_VALUE_HEADS * HEAD_SIZE))


def draw_queries(key, part):
    return paired_draw(key)[0].astype(jnp.bfloat16)


def draw_keys(key, part):
    return paired_draw(key)[1].astype(jnp.bfloat16)


def draw_span_order(key, part):
    base = jax.random.fold_in(key, 7171)
    order_key, flip_key = jax.random.split(base)
    pairs = jax.random.permutation(order_key, jnp.arange(N_CTX, dtype=jnp.int32))
    mirror = 2 * N_CTX - 1 - pairs
    flipped = jax.random.randint(flip_key, (N_CTX,), 0, 2, dtype=jnp.int32)
    first = jnp.where(flipped == 1, mirror, pairs)
    second = jnp.where(flipped == 1, pairs, mirror)
    return jnp.stack([first, second], axis=1).reshape(2 * N_CTX).astype(jnp.int32)


def block_scale(stream_key, shape, cuts, smallest, high):
    gain, own = 1.0, jax.random.fold_in(stream_key, 6)
    for dim, blocks in cuts:
        heights = jnp.exp(jax.random.uniform(jax.random.fold_in(own, dim), (blocks,), jnp.float32, smallest / len(cuts), high / len(cuts)))
        gain = gain * jnp.repeat(heights, shape[dim] // blocks).reshape([-1 if axis == dim else 1 for axis in range(len(shape))])
    return gain


def scatter_about(rng, extent, spread, most, pieces=(), kind=jnp.bfloat16):
    result = spread * jax.random.normal(rng, extent, jnp.float32)
    if pieces:
        result = result * block_scale(rng, extent, pieces, -0.22, 0.18)
    return jnp.clip(result, -most, most).astype(kind)


def setup_inputs(seed: int = 0) -> dict:
    splits = jax.random.split(jax.random.key(seed), 8)
    return {
        "queries": draw_queries(jax.random.fold_in(splits[7], 71), 0),
        "keys": draw_keys(jax.random.fold_in(splits[7], 71), 0),
        "values": scatter_about(splits[2], (SEQUENCE_LENGTH, KEY_VALUE_HEADS * HEAD_SIZE), 1.0, 6.0, ((0, 64), (1, 8))),
        "out_weight": scatter_about(splits[3], (QUERY_HEADS * HEAD_SIZE, D), (QUERY_HEADS * HEAD_SIZE) ** -0.5, 0.09375, ((0, 8),)),
        "residual": scatter_about(splits[4], (SEQUENCE_LENGTH, D), 0.25, 1.5, ((0, 64), (1, 8))),
        "norm_gain": jnp.clip(1.0 + 0.1 * jax.random.normal(splits[5], (D,), jnp.float32), 0.5, 1.5).astype(jnp.bfloat16),
        "span_order": draw_span_order(jax.random.fold_in(splits[7], 71), 0),
    }


def reference(queries, keys, values, out_weight, residual, norm_gain, span_order):
    total_spans = 2 * N_CTX
    span_rows = SEQUENCE_LENGTH // total_spans
    group_size = QUERY_HEADS // KEY_VALUE_HEADS
    scale = 1.0 / math.sqrt(HEAD_SIZE)
    slots = jnp.zeros((total_spans,), jnp.int32).at[span_order].set(jnp.arange(total_spans, dtype=jnp.int32))

    def map_to_positions(array):
        return array.reshape(total_spans, span_rows, array.shape[1])[slots].reshape(SEQUENCE_LENGTH, array.shape[1])
    every_query_row = map_to_positions(queries).astype(jnp.float32).reshape(SEQUENCE_LENGTH, KEY_VALUE_HEADS, group_size, HEAD_SIZE)
    every_key_row = map_to_positions(keys).astype(jnp.float32).reshape(SEQUENCE_LENGTH, KEY_VALUE_HEADS, HEAD_SIZE)
    every_value_row = map_to_positions(values).astype(jnp.float32).reshape(SEQUENCE_LENGTH, KEY_VALUE_HEADS, HEAD_SIZE)
    block_index = min(512, SEQUENCE_LENGTH)
    blocks = SEQUENCE_LENGTH // block_index

    def one_block(number):
        query_block = lax.dynamic_slice_in_dim(every_query_row, number * block_index, block_index, 0)
        query_pos = number * block_index + jnp.arange(block_index, dtype=jnp.int32)

        def step(other, state):
            running, total, accum = state
            key_block = lax.dynamic_slice_in_dim(every_key_row, other * block_index, block_index, 0)
            value_block = lax.dynamic_slice_in_dim(every_value_row, other * block_index, block_index, 0)
            key_pos = other * block_index + jnp.arange(block_index, dtype=jnp.int32)
            scores = jnp.einsum('qhgd,khd->qhgk', query_block, key_block) * scale
            allowed = (key_pos[None, :] <= query_pos[:, None])[:, None, None, :]
            scores = jnp.where(allowed, scores, -1e+30)
            newmax = jnp.maximum(running, lax.optimization_barrier(jnp.max(scores, axis=-1)))
            weights = jnp.where(allowed, jnp.exp(scores - newmax[..., None]), 0.0)
            fade = jnp.exp(running - newmax)
            total = total * fade + lax.optimization_barrier(jnp.sum(weights, axis=-1))
            rounded = lax.optimization_barrier(weights.astype(jnp.bfloat16)).astype(jnp.float32)
            accum = accum * fade[..., None] + jnp.einsum('qhgk,khd->qhgd', rounded, value_block)
            return (newmax, total, accum)
        start_offset = (jnp.full((block_index, KEY_VALUE_HEADS, group_size), -1e+30, jnp.float32), jnp.zeros((block_index, KEY_VALUE_HEADS, group_size), jnp.float32), jnp.zeros((block_index, KEY_VALUE_HEADS, group_size, HEAD_SIZE), jnp.float32))
        running, total, accum = lax.fori_loop(0, number + 1, step, start_offset)
        return accum / total[..., None]
    attended = lax.map(one_block, jnp.arange(blocks, dtype=jnp.int32))
    attended = attended.reshape(SEQUENCE_LENGTH, QUERY_HEADS * HEAD_SIZE).astype(jnp.bfloat16)
    attended = attended.reshape(total_spans, span_rows, QUERY_HEADS * HEAD_SIZE)[span_order].reshape(SEQUENCE_LENGTH, QUERY_HEADS * HEAD_SIZE)
    projected = jnp.dot(attended, out_weight, preferred_element_type=jnp.float32)
    hidden = (residual.astype(jnp.float32) + projected).astype(jnp.bfloat16)
    hidden_f = hidden.astype(jnp.float32)
    meansq = lax.optimization_barrier(jnp.mean(hidden_f * hidden_f, axis=1, keepdims=True))
    normed = hidden_f * lax.rsqrt(meansq + 1e-05) * norm_gain.astype(jnp.float32)[None, :]
    return normed.astype(jnp.bfloat16)
```

```python
import functools
import math

import jax
import jax.numpy as jnp
from jax import lax
from jax.experimental import pallas as pl
from jax.experimental.pallas import tpu as pltpu
from jax.sharding import Mesh, PartitionSpec as P

D = 4096
HEAD_SIZE = 128
EPSILON = 1e-05
SPAN = 64
HEADS = 4
NEG = -1e30
SCALE = 1.0 / math.sqrt(HEAD_SIZE)
LOG2E = math.log2(math.e)
STAT_ROWS = 16


def copies(shard, axis):
    stacked = jnp.broadcast_to(shard, (lax.axis_size(axis), *shard.shape))
    return lax.all_to_all(stacked, axis, split_axis=0, concat_axis=0, tiled=True)


def attention_kernel(qspan_ref, kspan_ref, q_ref, kv_ref, o_ref, vt_ref, s_ref):
    n_keys = kv_ref.shape[0]
    rows = HEADS * SPAN
    block = 256
    vt_ref[...] = kv_ref[:, HEAD_SIZE:].T
    diff = lax.broadcasted_iota(jnp.int32, (SPAN, rows), 0) - (
        lax.broadcasted_iota(jnp.int32, (SPAN, rows), 1) % SPAN
    )

    def tile(t, carry):
        peer = t // 2
        half = t % 2
        row0 = pl.multiple_of(half * SPAN, SPAN)
        qspan = qspan_ref[t]
        q = jnp.concatenate(
            [q_ref[peer, pl.ds(row0, SPAN), h * HEAD_SIZE : (h + 1) * HEAD_SIZE] for h in range(HEADS)],
            axis=0,
        )
        top = jnp.full((1, rows), NEG, jnp.float32)
        for b in range(n_keys // block):
            k = kv_ref[b * block : (b + 1) * block, :HEAD_SIZE]
            s = lax.dot_general(k, q, (((1,), (1,)), ((), ())), preferred_element_type=jnp.float32)
            for j in range(block // SPAN):
                n = b * (block // SPAN) + j
                limit = (qspan - kspan_ref[n]) * SPAN
                piece = jnp.where(diff <= limit, s[j * SPAN : (j + 1) * SPAN], NEG)
                s_ref[n * SPAN : (n + 1) * SPAN, :] = piece
                top = jnp.maximum(top, jnp.max(piece, axis=0, keepdims=True))
        total = jnp.zeros((1, rows), jnp.float32)
        acc = jnp.zeros((HEAD_SIZE, rows), jnp.float32)
        for b in range(n_keys // block):
            w = jnp.exp2((s_ref[b * block : (b + 1) * block, :] - top) * (SCALE * LOG2E))
            total = total + jnp.sum(w, axis=0, keepdims=True)
            acc = acc + jnp.dot(
                vt_ref[:, b * block : (b + 1) * block],
                w.astype(jnp.bfloat16),
                preferred_element_type=jnp.float32,
            )
        out = (acc / total).T.astype(jnp.bfloat16)
        for h in range(HEADS):
            o_ref[peer, pl.ds(row0, SPAN), h * HEAD_SIZE : (h + 1) * HEAD_SIZE] = out[h * SPAN : (h + 1) * SPAN]
        lse = top * SCALE + jnp.log(total)
        hi = lse.astype(jnp.bfloat16).astype(jnp.float32)
        mid = (lse - hi).astype(jnp.bfloat16).astype(jnp.float32)
        low = lse - hi - mid
        stats = jnp.concatenate([hi, mid, low, jnp.zeros((STAT_ROWS - 3, rows), jnp.float32)], axis=0)
        col0 = pl.multiple_of(half * rows, rows)
        o_ref[peer, 2 * SPAN :, pl.ds(col0, rows)] = stats.astype(jnp.bfloat16)
        return carry

    lax.fori_loop(0, 2 * q_ref.shape[0], tile, 0)


def attend(qspans, kspans, queries, kv):
    peers, local, width = queries.shape
    n_keys = kv.shape[0]
    vmem = pl.BlockSpec(memory_space=pltpu.VMEM)
    smem = pl.BlockSpec(memory_space=pltpu.SMEM)
    return pl.pallas_call(
        attention_kernel,
        out_shape=jax.ShapeDtypeStruct((peers, local + STAT_ROWS, width), jnp.bfloat16),
        in_specs=[smem, smem, vmem, vmem],
        out_specs=vmem,
        scratch_shapes=[
            pltpu.VMEM((HEAD_SIZE, n_keys), jnp.bfloat16),
            pltpu.VMEM((n_keys, HEADS * SPAN), jnp.float32),
        ],
        name="attend",
    )(qspans, kspans, queries, kv)


def combine_kernel(p_ref, o_ref):
    peers = p_ref.shape[0]
    width = p_ref.shape[2]
    lses = []
    for x in range(peers):
        st = p_ref[x, 2 * SPAN :, :].astype(jnp.float32)
        lses.append(st[0:1] + st[1:2] + st[2:3])
    top = functools.reduce(jnp.maximum, lses)
    ws = [jnp.exp(v - top) for v in lses]
    total = functools.reduce(jnp.add, ws)
    cols = jnp.concatenate([w / total for w in ws] + [jnp.zeros((8 - peers, width), jnp.float32)], axis=0).T
    for half in range(2):
        for h in range(HEADS):
            at = (half * HEADS + h) * SPAN
            out = jnp.zeros((SPAN, HEAD_SIZE), jnp.float32)
            for x in range(peers):
                part = p_ref[x, half * SPAN : (half + 1) * SPAN, h * HEAD_SIZE : (h + 1) * HEAD_SIZE]
                out = out + cols[at : at + SPAN, x : x + 1] * part.astype(jnp.float32)
            o_ref[half * SPAN : (half + 1) * SPAN, h * HEAD_SIZE : (h + 1) * HEAD_SIZE] = out.astype(jnp.bfloat16)


def combine(parts):
    peers, local, width = parts.shape
    vmem = pl.BlockSpec(memory_space=pltpu.VMEM)
    return pl.pallas_call(
        combine_kernel,
        out_shape=jax.ShapeDtypeStruct((2 * SPAN, width), jnp.bfloat16),
        in_specs=[vmem],
        out_specs=vmem,
        name="combine",
    )(parts)


def project_kernel(core_ref, own_ref, other_ref, w_ref, w2_ref, o_ref):
    out = jnp.dot(own_ref[...], w_ref[...], preferred_element_type=jnp.float32)
    out = out + jnp.dot(other_ref[...], w2_ref[...], preferred_element_type=jnp.float32)
    o_ref[0] = out.astype(jnp.bfloat16)


def project(core, own, other, weight, weight_other):
    rows, width = own.shape
    block = 512
    chips = weight.shape[1] // block // 2
    return pl.pallas_call(
        project_kernel,
        grid_spec=pltpu.PrefetchScalarGridSpec(
            num_scalar_prefetch=1,
            grid=(chips,),
            in_specs=[
                pl.BlockSpec((rows, width), lambda z, c: (0, 0)),
                pl.BlockSpec((rows, width), lambda z, c: (0, 0)),
                pl.BlockSpec((width, block), lambda z, c: (0, 2 * z + c[0])),
                pl.BlockSpec((width, block), lambda z, c: (0, 2 * z + c[0])),
            ],
            out_specs=pl.BlockSpec((1, rows, block), lambda z, c: (z, 0, 0)),
        ),
        out_shape=jax.ShapeDtypeStruct((chips, rows, block), jnp.bfloat16),
        name="project",
    )(core, own, other, weight, weight_other)


def per_device(queries, keys, values, out_weight, residual, norm_gain, span_order):
    y = lax.axis_index("y")
    zh = lax.axis_index("zh")
    x = lax.axis_index("x")
    core = lax.axis_index("c")
    spans = span_order.reshape(4, 4, 4, 2)
    qspans = lax.dynamic_slice(spans, (y, zh, 0, 0), (1, 1, 4, 2)).reshape(8)
    kspans = lax.dynamic_slice(spans, (0, 0, x, 0), (4, 4, 1, 2)).reshape(32)
    swap = [(0, 1), (1, 0)]
    weight_other = lax.ppermute(out_weight, "c", swap)
    kv = jnp.concatenate((keys, values), axis=1)
    kv = copies(kv, "zh")
    rows = kv.shape[0] * kv.shape[1]
    all_queries = copies(queries, "x")
    kv = copies(kv.reshape(rows, kv.shape[2]), "y")
    kv = kv.reshape(kv.shape[0] * rows, kv.shape[2])
    parts = attend(qspans, kspans, all_queries, kv)
    parts = lax.all_to_all(parts, "x", 0, 0, tiled=True)
    attended = combine(parts)
    attended_other = lax.ppermute(attended, "c", swap)
    partial_sums = project(core.reshape(1), attended, attended_other, out_weight, weight_other)
    share = lax.all_to_all(partial_sums, "zl", 0, 0, tiled=True)
    projected = jnp.sum(share.astype(jnp.float32), axis=0)
    hidden = (residual.astype(jnp.float32) + projected).astype(jnp.bfloat16)
    hidden_f = hidden.astype(jnp.float32)
    squares = copies(jnp.sum(hidden_f * hidden_f, axis=1)[None, :], ("zl", "c"))
    squares = jnp.sum(squares, axis=(0, 1))
    factor = lax.rsqrt(squares / D + EPSILON)
    normed = hidden_f * factor[:, None] * norm_gain.astype(jnp.float32)[None, :]
    return normed.astype(jnp.bfloat16)


def solution(mesh):
    fine = Mesh(mesh.devices.reshape(4, 4, 4, 4, 2), ("y", "zh", "x", "zl", "c"))
    ctx, tp = ("y", "zh", "x"), ("zl", "c")
    return jax.shard_map(
        per_device,
        mesh=fine,
        in_specs=(P(ctx, tp), P(ctx, tp), P(ctx, tp), P(tp, None), P(ctx, tp), P(tp), P()),
        out_specs=P(ctx, tp),
        check_vma=False,
    )
```

```python
import functools
import math

import jax
import jax.numpy as jnp
from jax import lax
from jax.experimental import pallas as pl
from jax.experimental.pallas import tpu as pltpu
from jax.sharding import Mesh, PartitionSpec as P


D = 4096
HEAD_SIZE = 128
EPSILON = 1e-05
SPAN = 64
HEADS = 4
NEG = -1e30
SCALE = 1.0 / math.sqrt(HEAD_SIZE)
LOG2E = math.log2(math.e)
STAT_ROWS = 16


def copies(shard, axis):
    stacked = jnp.broadcast_to(shard, (lax.axis_size(axis), *shard.shape))
    return lax.all_to_all(stacked, axis, split_axis=0, concat_axis=0, tiled=True)


def plan_kernel(dev_ref, span_ref, o_ref, flag_ref):
    dev = dev_ref[0]
    x = dev & 3
    row = dev >> 2
    n_spans = span_ref.shape[0]
    n_keys = n_spans // 4

    def clear(i, c):
        flag_ref[i] = -1
        return c

    lax.fori_loop(0, n_spans, clear, 0, unroll=16)

    def mark(i, c):
        slot = ((i >> 1) * 4 + x) * 2 + (i & 1)
        flag_ref[span_ref[slot]] = i
        return c

    lax.fori_loop(0, n_keys, mark, 0, unroll=8)

    def walk(p, n):
        f = flag_ref[p]
        o_ref[64 + n] = p
        o_ref[128 + n] = f
        n = n + jnp.where(f >= 0, 1, 0)
        flag_ref[p] = n
        return n

    lax.fori_loop(0, n_spans, walk, 0, unroll=8)
    for t in range(8):
        peer = (x + t // 2) & 3
        span = span_ref[(row * 4 + peer) * 2 + t % 2]
        o_ref[t] = span
        o_ref[8 + t] = jnp.maximum((flag_ref[span] + 3) >> 2, 1)
        if t % 2 == 0:
            o_ref[16 + t // 2] = peer


def plan(dev, span_order):
    smem = pl.BlockSpec(memory_space=pltpu.SMEM)
    return pl.pallas_call(
        plan_kernel,
        out_shape=jax.ShapeDtypeStruct((256,), jnp.int32),
        in_specs=[smem, smem],
        out_specs=smem,
        scratch_shapes=[pltpu.SMEM((128,), jnp.int32)],
        name="plan",
    )(dev, span_order)


def attention_kernel(tab_ref, q0_ref, q1_ref, q2_ref, q3_ref, kv_ref, o_ref, k_ref, v_ref, q_ref, s_ref, mx_ref, l_ref, acc_ref):
    rows = HEADS * SPAN
    block = 4 * SPAN
    lanes = HEAD_SIZE
    n_keys = kv_ref.shape[0]
    for i in range(n_keys // SPAN):
        src = pl.multiple_of(tab_ref[128 + i] * SPAN, SPAN)
        k_ref[i * SPAN : (i + 1) * SPAN, :] = kv_ref[pl.ds(src, SPAN), :HEAD_SIZE]
        v_ref[i * SPAN : (i + 1) * SPAN, :] = kv_ref[pl.ds(src, SPAN), HEAD_SIZE:]
    q_refs = (q0_ref, q1_ref, q2_ref, q3_ref)
    for peer in range(4):
        for half in range(2):
            for h in range(HEADS):
                at = ((peer * 2 + half) * HEADS + h) * SPAN
                q_ref[at : at + SPAN, :] = q_refs[peer][
                    half * SPAN : (half + 1) * SPAN, h * HEAD_SIZE : (h + 1) * HEAD_SIZE
                ]
    lane = lax.broadcasted_iota(jnp.int32, (rows, block), 1)
    diff = (lane % SPAN) - (lax.broadcasted_iota(jnp.int32, (rows, block), 0) % SPAN)
    lane_row = lax.broadcasted_iota(jnp.int32, (1, block), 1) // SPAN
    rest = n_keys // block - 1

    def pair(peer, mx_ref, l_ref, acc_ref, s_ref):
        nb = [tab_ref[8 + 2 * peer + half] for half in range(2)]
        work = [(0, nb[0] - 1), (1, nb[1] - 1)]
        for j in range(rest):
            second = j - (nb[0] - 1)
            half = jnp.where(second < 0, 0, jnp.where(second < nb[1] - 1, 1, 2))
            work.append((half, jnp.where(second < 0, j, jnp.where(second < nb[1] - 1, second, 0))))
        mx_ref[2] = jnp.zeros((rows, lanes), jnp.float32)
        for b, (half, kb) in enumerate(work):
            q_half = half if b < 2 else jnp.minimum(half, 1)
            q = q_ref[pl.ds(pl.multiple_of((peer * 2 + q_half) * rows, rows), rows), :]
            k = k_ref[pl.ds(pl.multiple_of(kb * block, block), block), :]
            s = lax.dot_general(q, k, (((1,), (1,)), ((), ())), preferred_element_type=jnp.float32)
            if b < 2:
                qspan = tab_ref[2 * peer + half]
                limits = [(qspan - tab_ref[64 + 4 * kb + j]) * SPAN for j in range(4)]
                limit = jnp.full((1, block), limits[0], jnp.int32)
                for j in range(1, 4):
                    limit = jnp.where(lane_row >= j, limits[j], limit)
                s = jnp.where(diff <= limit, s, NEG)
            s_ref[b] = s
            top = jnp.maximum(s[:, :lanes], s[:, lanes:])
            mx_ref[half] = top if b < 2 else jnp.maximum(mx_ref[half], top)
        for half in range(2):
            mx_ref[half] = jnp.broadcast_to(jnp.max(mx_ref[half], axis=1, keepdims=True), (rows, lanes))
        for b, (half, kb) in enumerate(work):
            m = mx_ref[half]
            s = s_ref[b]
            w0 = jnp.exp2((s[:, :lanes] - m) * (SCALE * LOG2E))
            w1 = jnp.exp2((s[:, lanes:] - m) * (SCALE * LOG2E))
            v = v_ref[pl.ds(pl.multiple_of(kb * block, block), block), :]
            w = jnp.concatenate([w0.astype(jnp.bfloat16), w1.astype(jnp.bfloat16)], axis=1)
            out = jnp.dot(w, v, preferred_element_type=jnp.float32)
            if b < 2:
                l_ref[half] = w0 + w1
                acc_ref[half] = out
            else:
                l_ref[half] = l_ref[half] + (w0 + w1)
                acc_ref[half] = acc_ref[half] + out
        dest = tab_ref[16 + peer]
        which = lax.broadcasted_iota(jnp.int32, (rows, lanes), 1)
        for half in range(2):
            total = jnp.broadcast_to(jnp.sum(l_ref[half], axis=1, keepdims=True), (rows, lanes))
            out = (acc_ref[half] * (1.0 / total)).astype(jnp.bfloat16)
            for h in range(HEADS):
                o_ref[dest, half * SPAN : (half + 1) * SPAN, h * HEAD_SIZE : (h + 1) * HEAD_SIZE] = out[
                    h * SPAN : (h + 1) * SPAN
                ]
            lse = mx_ref[half] * SCALE + jnp.log(total)
            hi = lse.astype(jnp.bfloat16).astype(jnp.float32)
            mid = (lse - hi).astype(jnp.bfloat16).astype(jnp.float32)
            low = lse - hi - mid
            stats = jnp.where(which == 0, hi, jnp.where(which == 1, mid, jnp.where(which == 2, low, 0.0)))
            o_ref[dest, 2 * SPAN :, half * rows : (half + 1) * rows] = stats.T[:STAT_ROWS].astype(jnp.bfloat16)

    for peer in range(4):
        pair(peer, mx_ref.at[peer], l_ref.at[peer], acc_ref.at[peer], s_ref.at[peer])


def attend(table, queries, kv):
    local, width = queries[0].shape
    peers = len(queries)
    n_keys = kv.shape[0]
    rows = HEADS * SPAN
    vmem = pl.BlockSpec(memory_space=pltpu.VMEM)
    smem = pl.BlockSpec(memory_space=pltpu.SMEM)
    return pl.pallas_call(
        attention_kernel,
        out_shape=jax.ShapeDtypeStruct((peers, local + STAT_ROWS, width), jnp.bfloat16),
        in_specs=[smem] + [vmem] * (peers + 1),
        out_specs=vmem,
        scratch_shapes=[
            pltpu.VMEM((n_keys, HEAD_SIZE), jnp.bfloat16),
            pltpu.VMEM((n_keys, HEAD_SIZE), jnp.bfloat16),
            pltpu.VMEM((peers * 2 * rows, HEAD_SIZE), jnp.bfloat16),
            pltpu.VMEM((peers, n_keys // rows + 1, rows, rows), jnp.float32),
            pltpu.VMEM((peers, 3, rows, HEAD_SIZE), jnp.float32),
            pltpu.VMEM((peers, 3, rows, HEAD_SIZE), jnp.float32),
            pltpu.VMEM((peers, 3, rows, HEAD_SIZE), jnp.float32),
        ],
        name="attend",
    )(table, *queries, kv)


def combine_kernel(p_ref, o_ref):
    peers = p_ref.shape[0]
    width = p_ref.shape[2]
    lses = []
    for x in range(peers):
        st = p_ref[x, 2 * SPAN :, :].astype(jnp.float32)
        lses.append(st[0:1] + st[1:2] + st[2:3])
    top = functools.reduce(jnp.maximum, lses)
    ws = [jnp.exp(v - top) for v in lses]
    total = functools.reduce(jnp.add, ws)
    cols = jnp.concatenate([w / total for w in ws] + [jnp.zeros((8 - peers, width), jnp.float32)], axis=0).T
    for half in range(2):
        for h in range(HEADS):
            at = (half * HEADS + h) * SPAN
            out = jnp.zeros((SPAN, HEAD_SIZE), jnp.float32)
            for x in range(peers):
                part = p_ref[x, half * SPAN : (half + 1) * SPAN, h * HEAD_SIZE : (h + 1) * HEAD_SIZE]
                out = out + cols[at : at + SPAN, x : x + 1] * part.astype(jnp.float32)
            o_ref[half * SPAN : (half + 1) * SPAN, h * HEAD_SIZE : (h + 1) * HEAD_SIZE] = out.astype(jnp.bfloat16)


def combine(parts):
    _, _, width = parts.shape
    vmem = pl.BlockSpec(memory_space=pltpu.VMEM)
    return pl.pallas_call(
        combine_kernel,
        out_shape=jax.ShapeDtypeStruct((2 * SPAN, width), jnp.bfloat16),
        in_specs=[vmem],
        out_specs=vmem,
        name="combine",
    )(parts)


def project_kernel(core_ref, own_ref, other_ref, w_ref, w2_ref, o_ref):
    out = jnp.dot(own_ref[...], w_ref[...], preferred_element_type=jnp.float32)
    out = out + jnp.dot(other_ref[...], w2_ref[...], preferred_element_type=jnp.float32)
    o_ref[0] = out.astype(jnp.bfloat16)


def project(core, own, other, weight, weight_other):
    rows, width = own.shape
    block = 512
    chips = weight.shape[1] // block // 2
    return pl.pallas_call(
        project_kernel,
        grid_spec=pltpu.PrefetchScalarGridSpec(
            num_scalar_prefetch=1,
            grid=(chips,),
            in_specs=[
                pl.BlockSpec((rows, width), lambda z, c: (0, 0)),
                pl.BlockSpec((rows, width), lambda z, c: (0, 0)),
                pl.BlockSpec((width, block), lambda z, c: (0, 2 * z + c[0])),
                pl.BlockSpec((width, block), lambda z, c: (0, 2 * z + c[0])),
            ],
            out_specs=pl.BlockSpec((1, rows, block), lambda z, c: (z, 0, 0)),
        ),
        out_shape=jax.ShapeDtypeStruct((chips, rows, block), jnp.bfloat16),
        name="project",
    )(core, own, other, weight, weight_other)


def per_device(queries, keys, values, out_weight, residual, norm_gain, span_order):
    y = lax.axis_index("y")
    zh = lax.axis_index("zh")
    x = lax.axis_index("x")
    core = lax.axis_index("c")
    swap = [(0, 1), (1, 0)]
    kv = copies(jnp.concatenate((keys, values), axis=1), "zh")
    rows = kv.shape[0] * kv.shape[1]
    qs = [queries] + [lax.ppermute(queries, "x", [(i, (i - d) % 4) for i in range(4)]) for d in (1, 2, 3)]
    weight_other = lax.ppermute(out_weight, "c", swap)
    kv = copies(kv.reshape(rows, kv.shape[2]), "y")
    table = plan(((y * 4 + zh) * 4 + x).reshape(1), span_order)
    kv = kv.reshape(kv.shape[0] * rows, kv.shape[2])
    parts = attend(table, qs, kv)
    parts = lax.all_to_all(parts, "x", 0, 0, tiled=True)
    attended = combine(parts)
    attended_other = lax.ppermute(attended, "c", swap)
    partial_sums = project(core.reshape(1), attended, attended_other, out_weight, weight_other)
    share = lax.all_to_all(partial_sums, "zl", 0, 0, tiled=True)
    projected = jnp.sum(share.astype(jnp.float32), axis=0)
    hidden = (residual.astype(jnp.float32) + projected).astype(jnp.bfloat16)
    hidden_f = hidden.astype(jnp.float32)
    squares = copies(jnp.sum(hidden_f * hidden_f, axis=1)[None, :], ("zl", "c"))
    squares = jnp.sum(squares, axis=(0, 1))
    factor = lax.rsqrt(squares / D + EPSILON)
    normed = hidden_f * factor[:, None] * norm_gain.astype(jnp.float32)[None, :]
    return normed.astype(jnp.bfloat16)


def solution(mesh):
    fine = Mesh(mesh.devices.reshape(4, 4, 4, 4, 2), ("y", "zh", "x", "zl", "c"))
    ctx, tp = ("y", "zh", "x"), ("zl", "c")
    return jax.shard_map(
        per_device,
        mesh=fine,
        in_specs=(P(ctx, tp), P(ctx, tp), P(ctx, tp), P(tp, None), P(ctx, tp), P(tp), P()),
        out_specs=P(ctx, tp),
        check_vma=False,
    )
```

```python
import functools
import math

import jax
import jax.numpy as jnp
from jax import lax
from jax.experimental import pallas as pl
from jax.experimental.pallas import tpu as pltpu
from jax.sharding import Mesh, PartitionSpec as P


D = 4096
HEAD_SIZE = 128
EPSILON = 1e-05
SPAN = 64
HEADS = 4
NEG = -1e30
SCALE = 1.0 / math.sqrt(HEAD_SIZE)
LOG2E = math.log2(math.e)
STAT_ROWS = 16


def copies(shard, axis):
    stacked = jnp.broadcast_to(shard, (lax.axis_size(axis), *shard.shape))
    return lax.all_to_all(stacked, axis, split_axis=0, concat_axis=0, tiled=True)


def in_vmem(array):
    return pltpu.with_memory_space_constraint(array, pltpu.VMEM)


def plan_kernel(dev_ref, span_ref, o_ref, flag_ref):
    dev = dev_ref[0]
    x = dev & 3
    row = dev >> 2
    n_spans = span_ref.shape[0]
    n_keys = n_spans // 4

    def clear(i, c):
        flag_ref[i] = -1
        return c

    lax.fori_loop(0, n_spans, clear, 0, unroll=16)

    def mark(i, c):
        slot = ((i >> 1) * 4 + x) * 2 + (i & 1)
        flag_ref[span_ref[slot]] = i
        return c

    lax.fori_loop(0, n_keys, mark, 0, unroll=8)

    def walk(p, n):
        f = flag_ref[p]
        o_ref[64 + n] = p
        o_ref[128 + n] = f
        n = n + jnp.where(f >= 0, 1, 0)
        flag_ref[p] = n
        return n

    lax.fori_loop(0, n_spans, walk, 0, unroll=8)
    for t in range(8):
        peer = (x + t // 2) & 3
        span = span_ref[(row * 4 + peer) * 2 + t % 2]
        o_ref[t] = span
        o_ref[8 + t] = jnp.maximum((flag_ref[span] + 3) >> 2, 1)
        if t % 2 == 0:
            o_ref[16 + t // 2] = peer


def plan(dev, span_order):
    smem = pl.BlockSpec(memory_space=pltpu.SMEM)
    return pl.pallas_call(
        plan_kernel,
        out_shape=jax.ShapeDtypeStruct((256,), jnp.int32),
        in_specs=[smem, smem],
        out_specs=smem,
        scratch_shapes=[pltpu.SMEM((128,), jnp.int32)],
        compiler_params=pltpu.CompilerParams(vmem_limit_bytes=1 * 2**20),
        name="plan",
    )(dev, span_order)


def attention_kernel(tab_ref, q0_ref, q1_ref, q2_ref, q3_ref, kv_ref, o_ref, k_ref, v_ref, q_ref, s_ref, mx_ref, l_ref, acc_ref):
    rows = HEADS * SPAN
    block = 4 * SPAN
    lanes = HEAD_SIZE
    n_keys = kv_ref.shape[0]
    for i in range(n_keys // SPAN):
        src = pl.multiple_of(tab_ref[128 + i] * SPAN, SPAN)
        k_ref[i * SPAN : (i + 1) * SPAN, :] = kv_ref[pl.ds(src, SPAN), :HEAD_SIZE]
        v_ref[i * SPAN : (i + 1) * SPAN, :] = kv_ref[pl.ds(src, SPAN), HEAD_SIZE:]
    q_refs = (q0_ref, q1_ref, q2_ref, q3_ref)
    for peer in range(4):
        for half in range(2):
            for h in range(HEADS):
                at = ((peer * 2 + half) * HEADS + h) * SPAN
                q_ref[at : at + SPAN, :] = q_refs[peer][
                    half * SPAN : (half + 1) * SPAN, h * HEAD_SIZE : (h + 1) * HEAD_SIZE
                ]
    lane = lax.broadcasted_iota(jnp.int32, (rows, block), 1)
    diff = (lane % SPAN) - (lax.broadcasted_iota(jnp.int32, (rows, block), 0) % SPAN)
    lane_row = lax.broadcasted_iota(jnp.int32, (1, block), 1) // SPAN
    rest = n_keys // block - 1

    def pair(peer, mx_ref, l_ref, acc_ref, s_ref):
        nb = [tab_ref[8 + 2 * peer + half] for half in range(2)]
        work = [(0, nb[0] - 1), (1, nb[1] - 1)]
        for j in range(rest):
            second = j - (nb[0] - 1)
            half = jnp.where(second < 0, 0, jnp.where(second < nb[1] - 1, 1, 2))
            work.append((half, jnp.where(second < 0, j, jnp.where(second < nb[1] - 1, second, 0))))
        mx_ref[2] = jnp.zeros((rows, lanes), jnp.float32)
        for b, (half, kb) in enumerate(work):
            q_half = half if b < 2 else jnp.minimum(half, 1)
            q = q_ref[pl.ds(pl.multiple_of((peer * 2 + q_half) * rows, rows), rows), :]
            k = k_ref[pl.ds(pl.multiple_of(kb * block, block), block), :]
            s = lax.dot_general(q, k, (((1,), (1,)), ((), ())), preferred_element_type=jnp.float32)
            if b < 2:
                qspan = tab_ref[2 * peer + half]
                limits = [(qspan - tab_ref[64 + 4 * kb + j]) * SPAN for j in range(4)]
                limit = jnp.full((1, block), limits[0], jnp.int32)
                for j in range(1, 4):
                    limit = jnp.where(lane_row >= j, limits[j], limit)
                s = jnp.where(diff <= limit, s, NEG)
            s_ref[b] = s
            top = jnp.maximum(s[:, :lanes], s[:, lanes:])
            mx_ref[half] = top if b < 2 else jnp.maximum(mx_ref[half], top)
        for half in range(2):
            mx_ref[half] = jnp.broadcast_to(jnp.max(mx_ref[half], axis=1, keepdims=True), (rows, lanes))
        for b, (half, kb) in enumerate(work):
            m = mx_ref[half]
            s = s_ref[b]
            w0 = jnp.exp2((s[:, :lanes] - m) * (SCALE * LOG2E))
            w1 = jnp.exp2((s[:, lanes:] - m) * (SCALE * LOG2E))
            v = v_ref[pl.ds(pl.multiple_of(kb * block, block), block), :]
            w = jnp.concatenate([w0.astype(jnp.bfloat16), w1.astype(jnp.bfloat16)], axis=1)
            out = jnp.dot(w, v, preferred_element_type=jnp.float32)
            if b < 2:
                l_ref[half] = w0 + w1
                acc_ref[half] = out
            else:
                l_ref[half] = l_ref[half] + (w0 + w1)
                acc_ref[half] = acc_ref[half] + out
        dest = tab_ref[16 + peer]
        which = lax.broadcasted_iota(jnp.int32, (rows, lanes), 1)
        for half in range(2):
            total = jnp.broadcast_to(jnp.sum(l_ref[half], axis=1, keepdims=True), (rows, lanes))
            out = (acc_ref[half] * (1.0 / total)).astype(jnp.bfloat16)
            for h in range(HEADS):
                o_ref[dest, half * SPAN : (half + 1) * SPAN, h * HEAD_SIZE : (h + 1) * HEAD_SIZE] = out[
                    h * SPAN : (h + 1) * SPAN
                ]
            lse = mx_ref[half] * SCALE + jnp.log(total)
            hi = lse.astype(jnp.bfloat16).astype(jnp.float32)
            mid = (lse - hi).astype(jnp.bfloat16).astype(jnp.float32)
            low = lse - hi - mid
            stats = jnp.where(which == 0, hi, jnp.where(which == 1, mid, jnp.where(which == 2, low, 0.0)))
            o_ref[dest, 2 * SPAN :, half * rows : (half + 1) * rows] = stats.T[:STAT_ROWS].astype(jnp.bfloat16)

    for peer in range(4):
        pair(peer, mx_ref.at[peer], l_ref.at[peer], acc_ref.at[peer], s_ref.at[peer])


def attend(table, queries, kv):
    local, width = queries[0].shape
    peers = len(queries)
    n_keys = kv.shape[0]
    rows = HEADS * SPAN
    vmem = pl.BlockSpec(memory_space=pltpu.VMEM)
    smem = pl.BlockSpec(memory_space=pltpu.SMEM)
    return pl.pallas_call(
        attention_kernel,
        out_shape=pltpu.VMEM((peers, local + STAT_ROWS, width), jnp.bfloat16),
        in_specs=[smem] + [vmem] * (peers + 1),
        out_specs=vmem,
        scratch_shapes=[
            pltpu.VMEM((n_keys, HEAD_SIZE), jnp.bfloat16),
            pltpu.VMEM((n_keys, HEAD_SIZE), jnp.bfloat16),
            pltpu.VMEM((peers * 2 * rows, HEAD_SIZE), jnp.bfloat16),
            pltpu.VMEM((peers, n_keys // rows + 1, rows, rows), jnp.float32),
            pltpu.VMEM((peers, 3, rows, HEAD_SIZE), jnp.float32),
            pltpu.VMEM((peers, 3, rows, HEAD_SIZE), jnp.float32),
            pltpu.VMEM((peers, 3, rows, HEAD_SIZE), jnp.float32),
        ],
        compiler_params=pltpu.CompilerParams(vmem_limit_bytes=24 * 2**20),
        name="attend",
    )(table, *[in_vmem(a) for a in queries], in_vmem(kv))


def combine_kernel(p_ref, o_ref):
    peers = p_ref.shape[0]
    width = p_ref.shape[2]
    lses = []
    for x in range(peers):
        st = p_ref[x, 2 * SPAN :, :].astype(jnp.float32)
        lses.append(st[0:1] + st[1:2] + st[2:3])
    top = functools.reduce(jnp.maximum, lses)
    ws = [jnp.exp(v - top) for v in lses]
    total = functools.reduce(jnp.add, ws)
    cols = jnp.concatenate([w / total for w in ws] + [jnp.zeros((8 - peers, width), jnp.float32)], axis=0).T
    for half in range(2):
        for h in range(HEADS):
            at = (half * HEADS + h) * SPAN
            out = jnp.zeros((SPAN, HEAD_SIZE), jnp.float32)
            for x in range(peers):
                part = p_ref[x, half * SPAN : (half + 1) * SPAN, h * HEAD_SIZE : (h + 1) * HEAD_SIZE]
                out = out + cols[at : at + SPAN, x : x + 1] * part.astype(jnp.float32)
            o_ref[half * SPAN : (half + 1) * SPAN, h * HEAD_SIZE : (h + 1) * HEAD_SIZE] = out.astype(jnp.bfloat16)


def combine(parts):
    _, _, width = parts.shape
    vmem = pl.BlockSpec(memory_space=pltpu.VMEM)
    return pl.pallas_call(
        combine_kernel,
        out_shape=pltpu.VMEM((2 * SPAN, width), jnp.bfloat16),
        in_specs=[vmem],
        out_specs=vmem,
        compiler_params=pltpu.CompilerParams(vmem_limit_bytes=4 * 2**20),
        name="combine",
    )(in_vmem(parts))


def split_kernel(core_ref, w_ref, keep_ref, send_ref, sem):
    core = core_ref[0]
    block = 512
    moves = []
    for z in range(keep_ref.shape[1] // block):
        for ref, which in ((keep_ref, core), (send_ref, 1 - core)):
            at = pl.multiple_of((2 * z + which) * block, block)
            src = w_ref.at[:, pl.ds(at, block)]
            moves.append(pltpu.make_async_copy(src, ref.at[:, z * block : (z + 1) * block], sem.at[len(moves)]))
    for move in moves:
        move.start()
    for move in moves:
        move.wait()


def split(core, weight):
    rows, width = weight.shape
    vmem = pl.BlockSpec(memory_space=pltpu.VMEM)
    smem = pl.BlockSpec(memory_space=pltpu.SMEM)
    half = pltpu.VMEM((rows, width // 2), jnp.bfloat16)
    return pl.pallas_call(
        split_kernel,
        in_specs=[smem, pl.BlockSpec(memory_space=pltpu.HBM)],
        out_specs=(vmem, vmem),
        out_shape=(half, half),
        scratch_shapes=[pltpu.SemaphoreType.DMA((8,))],
        compiler_params=pltpu.CompilerParams(vmem_limit_bytes=2 * 2**20),
        name="split",
    )(core, pltpu.with_memory_space_constraint(weight, pltpu.HBM))


def project_kernel(own_ref, other_ref, w_ref, w2_ref, o_ref):
    chips, _, block = o_ref.shape
    own = own_ref[...]
    other = other_ref[...]
    for z in range(chips):
        cols = slice(z * block, (z + 1) * block)
        out = jnp.dot(own, w_ref[:, cols], preferred_element_type=jnp.float32)
        out = out + jnp.dot(other, w2_ref[:, cols], preferred_element_type=jnp.float32)
        o_ref[z] = out.astype(jnp.bfloat16)


def project(own, other, weight, weight_other):
    rows = own.shape[0]
    block = 512
    vmem = pl.BlockSpec(memory_space=pltpu.VMEM)
    return pl.pallas_call(
        project_kernel,
        in_specs=[vmem] * 4,
        out_specs=vmem,
        out_shape=pltpu.VMEM((weight.shape[1] // block, rows, block), jnp.bfloat16),
        compiler_params=pltpu.CompilerParams(vmem_limit_bytes=4 * 2**20),
        name="project",
    )(*[in_vmem(a) for a in (own, other, weight, weight_other)])


def per_device(queries, keys, values, out_weight, residual, norm_gain, span_order):
    y = lax.axis_index("y")
    zh = lax.axis_index("zh")
    x = lax.axis_index("x")
    core = lax.axis_index("c")
    swap = [(0, 1), (1, 0)]
    kv = copies(jnp.concatenate((keys, values), axis=1), "zh")
    rows = kv.shape[0] * kv.shape[1]
    qs = [queries] + [lax.ppermute(queries, "x", [(i, (i - d) % 4) for i in range(4)]) for d in (1, 2, 3)]
    kv = copies(kv.reshape(rows, kv.shape[2]), "y")
    weight, weight_send = split(core.reshape(1), out_weight)
    weight_other = lax.ppermute(weight_send, "c", swap)
    table = plan(((y * 4 + zh) * 4 + x).reshape(1), span_order)
    kv = kv.reshape(kv.shape[0] * rows, kv.shape[2])
    parts = attend(table, qs, kv)
    parts = lax.all_to_all(parts, "x", 0, 0, tiled=True)
    attended = combine(parts)
    attended_other = lax.ppermute(attended, "c", swap)
    partial_sums = project(attended, attended_other, weight, weight_other)
    share = lax.all_to_all(partial_sums, "zl", 0, 0, tiled=True)
    projected = jnp.sum(share.astype(jnp.float32), axis=0)
    hidden = (residual.astype(jnp.float32) + projected).astype(jnp.bfloat16)
    hidden_f = hidden.astype(jnp.float32)
    squares = copies(jnp.sum(hidden_f * hidden_f, axis=1)[None, :], ("zl", "c"))
    squares = jnp.sum(squares, axis=(0, 1))
    factor = lax.rsqrt(squares / D + EPSILON)
    normed = hidden_f * factor[:, None] * norm_gain.astype(jnp.float32)[None, :]
    return normed.astype(jnp.bfloat16)


def solution(mesh):
    fine = Mesh(mesh.devices.reshape(4, 4, 4, 4, 2), ("y", "zh", "x", "zl", "c"))
    ctx, tp = ("y", "zh", "x"), ("zl", "c")
    return jax.shard_map(
        per_device,
        mesh=fine,
        in_specs=(P(ctx, tp), P(ctx, tp), P(ctx, tp), P(tp, None), P(ctx, tp), P(tp), P()),
        out_specs=P(ctx, tp),
        check_vma=False,
    )
```

```python
import functools
import math

import jax
import jax.numpy as jnp
from jax import lax
from jax.experimental import pallas as pl
from jax.experimental.pallas import tpu as pltpu
from jax.sharding import Mesh, PartitionSpec as P


D = 4096
HEAD_SIZE = 128
EPSILON = 1e-05
SPAN = 64
HEADS = 4
NEG = -1e30
SCALE = 1.0 / math.sqrt(HEAD_SIZE)
LOG2E = math.log2(math.e)
STAT_ROWS = 16


def in_vmem(array):
    return pltpu.with_memory_space_constraint(array, pltpu.VMEM)


def spread_kernel(*refs):
    o_ref = refs[-1]
    at = 0
    for ref in refs[:-1]:
        part = ref[...]
        for i in range(o_ref.shape[0]):
            o_ref[i, :, at : at + part.shape[1]] = part
        at += part.shape[1]


def spread(arrays, copies):
    rows = arrays[0].shape[0]
    width = sum(a.shape[1] for a in arrays)
    vmem = pl.BlockSpec(memory_space=pltpu.VMEM)
    return pl.pallas_call(
        spread_kernel,
        in_specs=[vmem] * len(arrays),
        out_specs=vmem,
        out_shape=pltpu.VMEM((copies, rows, width), arrays[0].dtype),
        compiler_params=pltpu.CompilerParams(vmem_limit_bytes=2 * 2**20),
        name="spread",
    )(*arrays)


def plan_kernel(dev_ref, span_ref, o_ref, flag_ref):
    dev = dev_ref[0]
    x = dev & 3
    row = dev >> 2
    n_spans = span_ref.shape[0]
    n_keys = n_spans // 4

    def clear(i, c):
        flag_ref[i] = -1
        return c

    lax.fori_loop(0, n_spans, clear, 0, unroll=16)

    def mark(i, c):
        slot = ((i >> 1) * 4 + x) * 2 + (i & 1)
        flag_ref[span_ref[slot]] = i
        return c

    lax.fori_loop(0, n_keys, mark, 0, unroll=8)

    def walk(p, n):
        f = flag_ref[p]
        o_ref[64 + n] = p
        o_ref[128 + n] = f
        n = n + jnp.where(f >= 0, 1, 0)
        flag_ref[p] = n
        return n

    lax.fori_loop(0, n_spans, walk, 0, unroll=8)
    for t in range(8):
        peer = (x + t // 2) & 3
        span = span_ref[(row * 4 + peer) * 2 + t % 2]
        o_ref[t] = span
        o_ref[8 + t] = jnp.maximum((flag_ref[span] + 3) >> 2, 1)
        if t % 2 == 0:
            o_ref[16 + t // 2] = peer


def plan(dev, span_order):
    smem = pl.BlockSpec(memory_space=pltpu.SMEM)
    return pl.pallas_call(
        plan_kernel,
        out_shape=jax.ShapeDtypeStruct((256,), jnp.int32),
        in_specs=[smem, smem],
        out_specs=smem,
        scratch_shapes=[pltpu.SMEM((128,), jnp.int32)],
        compiler_params=pltpu.CompilerParams(vmem_limit_bytes=1 * 2**20),
        name="plan",
    )(dev, span_order)


def attention_kernel(tab_ref, q0_ref, q1_ref, q2_ref, q3_ref, kv_ref, o_ref, k_ref, v_ref, q_ref, s_ref, mx_ref, l_ref, acc_ref):
    rows = HEADS * SPAN
    block = 4 * SPAN
    lanes = HEAD_SIZE
    n_keys = kv_ref.shape[0]
    for i in range(n_keys // SPAN):
        src = pl.multiple_of(tab_ref[128 + i] * SPAN, SPAN)
        k_ref[i * SPAN : (i + 1) * SPAN, :] = kv_ref[pl.ds(src, SPAN), :HEAD_SIZE]
        v_ref[i * SPAN : (i + 1) * SPAN, :] = kv_ref[pl.ds(src, SPAN), HEAD_SIZE:]
    q_refs = (q0_ref, q1_ref, q2_ref, q3_ref)
    for peer in range(4):
        for half in range(2):
            for h in range(HEADS):
                at = ((peer * 2 + half) * HEADS + h) * SPAN
                q_ref[at : at + SPAN, :] = q_refs[peer][
                    half * SPAN : (half + 1) * SPAN, h * HEAD_SIZE : (h + 1) * HEAD_SIZE
                ]
    lane = lax.broadcasted_iota(jnp.int32, (rows, block), 1)
    diff = (lane % SPAN) - (lax.broadcasted_iota(jnp.int32, (rows, block), 0) % SPAN)
    lane_row = lax.broadcasted_iota(jnp.int32, (1, block), 1) // SPAN
    rest = n_keys // block - 1

    def pair(peer, mx_ref, l_ref, acc_ref, s_ref):
        nb = [tab_ref[8 + 2 * peer + half] for half in range(2)]
        work = [(0, nb[0] - 1), (1, nb[1] - 1)]
        for j in range(rest):
            second = j - (nb[0] - 1)
            half = jnp.where(second < 0, 0, jnp.where(second < nb[1] - 1, 1, 2))
            work.append((half, jnp.where(second < 0, j, jnp.where(second < nb[1] - 1, second, 0))))
        mx_ref[2] = jnp.zeros((rows, lanes), jnp.float32)
        for b, (half, kb) in enumerate(work):
            q_half = half if b < 2 else jnp.minimum(half, 1)
            q = q_ref[pl.ds(pl.multiple_of((peer * 2 + q_half) * rows, rows), rows), :]
            k = k_ref[pl.ds(pl.multiple_of(kb * block, block), block), :]
            if b < 2:
                qspan = tab_ref[2 * peer + half]
                limits = [(qspan - tab_ref[64 + 4 * kb + j]) * SPAN for j in range(4)]
                limit = jnp.full((1, block), limits[0], jnp.int32)
                for j in range(1, 4):
                    limit = jnp.where(lane_row >= j, limits[j], limit)
            for r in range(0, rows, 128):
                part = slice(r, r + 128)
                s = lax.dot_general(q[part], k, (((1,), (1,)), ((), ())), preferred_element_type=jnp.float32)
                if b < 2:
                    s = jnp.where(diff[part] <= limit, s, NEG)
                s_ref[b, part] = s
                top = jnp.maximum(s[:, :lanes], s[:, lanes:])
                mx_ref[half, part] = top if b < 2 else jnp.maximum(mx_ref[half, part], top)
        for half in range(2):
            mx_ref[half] = jnp.broadcast_to(jnp.max(mx_ref[half], axis=1, keepdims=True), (rows, lanes))
        for b, (half, kb) in enumerate(work):
            v = v_ref[pl.ds(pl.multiple_of(kb * block, block), block), :]
            for r in range(0, rows, 128):
                part = slice(r, r + 128)
                m = mx_ref[half, part]
                w0 = jnp.exp2((s_ref[b, part, :lanes] - m) * (SCALE * LOG2E))
                w1 = jnp.exp2((s_ref[b, part, lanes:] - m) * (SCALE * LOG2E))
                w = jnp.concatenate([w0.astype(jnp.bfloat16), w1.astype(jnp.bfloat16)], axis=1)
                out = jnp.dot(w, v, preferred_element_type=jnp.float32)
                if b < 2:
                    l_ref[half, part] = w0 + w1
                    acc_ref[half, part] = out
                else:
                    l_ref[half, part] = l_ref[half, part] + (w0 + w1)
                    acc_ref[half, part] = acc_ref[half, part] + out
        dest = tab_ref[16 + peer]
        which = lax.broadcasted_iota(jnp.int32, (rows, lanes), 1)
        for half in range(2):
            total = jnp.broadcast_to(jnp.sum(l_ref[half], axis=1, keepdims=True), (rows, lanes))
            out = (acc_ref[half] * (1.0 / total)).astype(jnp.bfloat16)
            for h in range(HEADS):
                o_ref[dest, half * SPAN : (half + 1) * SPAN, h * HEAD_SIZE : (h + 1) * HEAD_SIZE] = out[
                    h * SPAN : (h + 1) * SPAN
                ]
            lse = mx_ref[half] * SCALE + jnp.log(total)
            hi = lse.astype(jnp.bfloat16).astype(jnp.float32)
            mid = (lse - hi).astype(jnp.bfloat16).astype(jnp.float32)
            low = lse - hi - mid
            stats = jnp.where(which == 0, hi, jnp.where(which == 1, mid, jnp.where(which == 2, low, 0.0)))
            o_ref[dest, 2 * SPAN :, half * rows : (half + 1) * rows] = stats.T[:STAT_ROWS].astype(jnp.bfloat16)

    for peer in range(4):
        pair(peer, mx_ref.at[peer], l_ref.at[peer], acc_ref.at[peer], s_ref.at[peer])


def attend(table, queries, kv):
    local, width = queries[0].shape
    peers = len(queries)
    n_keys = kv.shape[0]
    rows = HEADS * SPAN
    vmem = pl.BlockSpec(memory_space=pltpu.VMEM)
    smem = pl.BlockSpec(memory_space=pltpu.SMEM)
    return pl.pallas_call(
        attention_kernel,
        out_shape=pltpu.VMEM((peers, local + STAT_ROWS, width), jnp.bfloat16),
        in_specs=[smem] + [vmem] * (peers + 1),
        out_specs=vmem,
        scratch_shapes=[
            pltpu.VMEM((n_keys, HEAD_SIZE), jnp.bfloat16),
            pltpu.VMEM((n_keys, HEAD_SIZE), jnp.bfloat16),
            pltpu.VMEM((peers * 2 * rows, HEAD_SIZE), jnp.bfloat16),
            pltpu.VMEM((peers, n_keys // rows + 1, rows, rows), jnp.float32),
            pltpu.VMEM((peers, 3, rows, HEAD_SIZE), jnp.float32),
            pltpu.VMEM((peers, 3, rows, HEAD_SIZE), jnp.float32),
            pltpu.VMEM((peers, 3, rows, HEAD_SIZE), jnp.float32),
        ],
        compiler_params=pltpu.CompilerParams(vmem_limit_bytes=24 * 2**20),
        name="attend",
    )(table, *[in_vmem(a) for a in queries], in_vmem(kv))


def combine_kernel(p_ref, o_ref):
    peers = p_ref.shape[0]
    width = p_ref.shape[2]
    lses = []
    for x in range(peers):
        st = p_ref[x, 2 * SPAN :, :].astype(jnp.float32)
        lses.append(st[0:1] + st[1:2] + st[2:3])
    top = functools.reduce(jnp.maximum, lses)
    ws = [jnp.exp(v - top) for v in lses]
    total = functools.reduce(jnp.add, ws)
    cols = jnp.concatenate([w / total for w in ws] + [jnp.zeros((8 - peers, width), jnp.float32)], axis=0).T
    for half in range(2):
        for h in range(HEADS):
            at = (half * HEADS + h) * SPAN
            out = jnp.zeros((SPAN, HEAD_SIZE), jnp.float32)
            for x in range(peers):
                part = p_ref[x, half * SPAN : (half + 1) * SPAN, h * HEAD_SIZE : (h + 1) * HEAD_SIZE]
                out = out + cols[at : at + SPAN, x : x + 1] * part.astype(jnp.float32)
            o_ref[half * SPAN : (half + 1) * SPAN, h * HEAD_SIZE : (h + 1) * HEAD_SIZE] = out.astype(jnp.bfloat16)


def combine(parts):
    _, _, width = parts.shape
    vmem = pl.BlockSpec(memory_space=pltpu.VMEM)
    return pl.pallas_call(
        combine_kernel,
        out_shape=pltpu.VMEM((2 * SPAN, width), jnp.bfloat16),
        in_specs=[vmem],
        out_specs=vmem,
        compiler_params=pltpu.CompilerParams(vmem_limit_bytes=4 * 2**20),
        name="combine",
    )(in_vmem(parts))


def columns_kernel(blocks, at_ref, w_ref, w2_ref, o_ref, o2_ref, sem):
    core = at_ref[0] & 1
    place = at_ref[0] >> 1
    width = o_ref.shape[1] // len(blocks)
    moves = []
    for i, d in enumerate(blocks):
        at = pl.multiple_of((2 * (place ^ d) + core) * width, width)
        for src, dst in ((w_ref, o_ref), (w2_ref, o2_ref)):
            dst = dst.at[:, i * width : (i + 1) * width]
            moves.append(pltpu.make_async_copy(src.at[:, pl.ds(at, width)], dst, sem.at[len(moves)]))
    for move in moves:
        move.start()
    for move in moves:
        move.wait()


def columns(blocks, place, weight, weight_other):
    rows = weight.shape[0]
    vmem = pl.BlockSpec(memory_space=pltpu.VMEM)
    hbm = pl.BlockSpec(memory_space=pltpu.HBM)
    return pl.pallas_call(
        functools.partial(columns_kernel, blocks),
        in_specs=[pl.BlockSpec(memory_space=pltpu.SMEM), hbm, hbm],
        out_specs=(vmem, vmem),
        out_shape=(pltpu.VMEM((rows, 512 * len(blocks)), jnp.bfloat16),) * 2,
        scratch_shapes=[pltpu.SemaphoreType.DMA((2 * len(blocks),))],
        compiler_params=pltpu.CompilerParams(vmem_limit_bytes=2 * 2**20),
        name="columns",
    )(place, *[pltpu.with_memory_space_constraint(w, pltpu.HBM) for w in (weight, weight_other)])


def project_kernel(own_ref, other_ref, w_ref, w2_ref, *o_refs):
    width = o_refs[0].shape[1]
    own = own_ref[...]
    other = other_ref[...]
    for i, o_ref in enumerate(o_refs):
        cols = slice(i * width, (i + 1) * width)
        out = jnp.dot(own, w_ref[:, cols], preferred_element_type=jnp.float32)
        out = out + jnp.dot(other, w2_ref[:, cols], preferred_element_type=jnp.float32)
        o_ref[...] = out.astype(o_ref.dtype)


def project(blocks, own, other, weight, weight_other):
    rows = own.shape[0]
    vmem = pl.BlockSpec(memory_space=pltpu.VMEM)
    return pl.pallas_call(
        project_kernel,
        in_specs=[vmem] * 4,
        out_specs=tuple(vmem for d in blocks),
        out_shape=tuple(pltpu.VMEM((rows, 512), jnp.bfloat16 if d else jnp.float32) for d in blocks),
        compiler_params=pltpu.CompilerParams(vmem_limit_bytes=4 * 2**20),
        name="project",
    )(*[in_vmem(a) for a in (own, other, weight, weight_other)])


def total_kernel(p0_ref, p1_ref, p2_ref, p3_ref, r_ref, h_ref, s_ref):
    total = p0_ref[...]
    for ref in (p1_ref, p2_ref, p3_ref):
        total = total + ref[...].astype(jnp.float32)
    hidden = (r_ref[...].astype(jnp.float32) + total).astype(jnp.bfloat16)
    h_ref[...] = hidden
    hidden = hidden.astype(jnp.float32)
    squares = jnp.sum(hidden * hidden, axis=1, keepdims=True)
    row = jnp.broadcast_to(squares, (squares.shape[0], 128)).T[:1]
    for i in range(s_ref.shape[0]):
        s_ref[i] = row


def total(parts, residual):
    rows, width = residual.shape
    vmem = pl.BlockSpec(memory_space=pltpu.VMEM)
    return pl.pallas_call(
        total_kernel,
        in_specs=[vmem] * 5,
        out_specs=(vmem, vmem),
        out_shape=(pltpu.VMEM((rows, width), jnp.bfloat16), pltpu.VMEM((8, 1, rows), jnp.float32)),
        compiler_params=pltpu.CompilerParams(vmem_limit_bytes=4 * 2**20),
        name="total",
    )(*[in_vmem(a) for a in (*parts, residual)])


def per_device(queries, keys, values, out_weight, residual, norm_gain, span_order):
    y = lax.axis_index("y")
    zh = lax.axis_index("zh")
    x = lax.axis_index("x")
    core = lax.axis_index("c")
    swap = [(0, 1), (1, 0)]
    shift = lambda a, axis, d: lax.ppermute(a, axis, [(i, (i - d) % 4) for i in range(4)])
    kv = jnp.concatenate((keys, values), axis=1)
    kv = lax.all_to_all(jnp.broadcast_to(kv, (4, *kv.shape)), "zh", 0, 0, tiled=True)
    qs = [queries] + [shift(queries, "x", d) for d in (1, 2, 3)]
    kv = lax.all_to_all(spread((in_vmem(kv.reshape(-1, kv.shape[2])),), 4), "y", 0, 0, tiled=True)
    weight_other = lax.ppermute(out_weight, "c", swap)
    table = plan(((y * 4 + zh) * 4 + x).reshape(1), span_order)
    parts = attend(table, qs, kv.reshape(-1, kv.shape[2]))
    parts = lax.all_to_all(parts, "x", 0, 0, tiled=True)
    place = (2 * lax.axis_index("zl") + core).reshape(1)
    far_weights = columns((2, 3), place, out_weight, weight_other)
    attended = combine(parts)
    attended_other = lax.ppermute(attended, "c", swap)
    across = lambda a, d: lax.ppermute(a, "zl", [(i, i ^ d) for i in range(4)])
    far2, far3 = project((2, 3), attended, attended_other, *far_weights)
    far2 = across(far2, 2)
    far3 = across(far3, 3)
    near_weights = columns((0, 1), place, out_weight, weight_other)
    own, near = project((0, 1), attended, attended_other, *near_weights)
    near = across(near, 1)
    hidden, squares = total((own, near, far2, far3), residual)
    hidden_f = hidden.astype(jnp.float32)
    squares = lax.all_to_all(squares, ("zl", "c"), 0, 0, tiled=True)
    squares = jnp.sum(squares, axis=(0, 1))
    factor = lax.rsqrt(squares / D + EPSILON)
    normed = hidden_f * factor[:, None] * norm_gain.astype(jnp.float32)[None, :]
    return normed.astype(jnp.bfloat16)


def solution(mesh):
    fine = Mesh(mesh.devices.reshape(4, 4, 4, 4, 2), ("y", "zh", "x", "zl", "c"))
    ctx, tp = ("y", "zh", "x"), ("zl", "c")
    return jax.shard_map(
        per_device,
        mesh=fine,
        in_specs=(P(ctx, tp), P(ctx, tp), P(ctx, tp), P(tp, None), P(ctx, tp), P(tp), P()),
        out_specs=P(ctx, tp),
        check_vma=False,
    )
```
